32 devices in a mesh: section: 4 (over x, core), head: 8 (over z, y).
Axes of the slice: x: 2, y: 2, z: 4, core: 2. Of those that a mesh axis runs over, the one named last changes fastest.
Arguments:
- hidden: float32 [4, 32, 7168], P(None, 'section'), may hold values from -6 to 6
- norm_gain: float32 [7168], replicated, may hold values from 0.5 to 1.5
- router: bfloat16 [7168, 8], replicated, may hold values from -0.0625 to 0.0625
- key_value_weight: bfloat16 [7168, 256], replicated, may hold values from -0.0625 to 0.0625
- query_master: float32 [7168, 1024], P('section', 'head'), may hold values from -0.0625 to 0.0625
- output_master: float32 [7168, 1024], P('section', 'head'), may hold values from -1 to 1
- key_value_cache: bfloat16 [32, 256, 256], P('section', 'head'), may hold values from -480 to 480
- lengths: int32 [32], P('section'), may hold values from 64 to 256
- routes: int32 [4, 32, 4], P(None, 'section'), may hold values from 0 to 7, all different within a row
Outputs:
- handed_on: float32 [4, 32, 7168], P(None, 'section', 'head')
The draws below stay inside these ranges and needn't reach their ends.
All inputs are finite; a program needn't handle non-finite values.
Results may differ from the reference program's by a relative error of at most 0.012.
The reference program's roundings to bfloat16 on the way (of `normed`, `fresh_pairs`, `queries` and `attended`) count: a program that leaves them out, or rounds other values in their place, can miss the bound.
Values may be sent and summed in bfloat16 or wider, within the bound.
No kernel may reach another device: no remote copies, remote signals or barrier semaphores. Data moves between devices by JAX's collectives and lax.ppermute only.
A program may use at most 64 MiB of HBM per device.

```python
import math
import jax
import jax.numpy as jnp
from jax import lax

D = 7168
HEAD = 128
TOPK = 4
STEPS = 4
ROWS_DEV = 8
EXPERTS = 8
ROWS = 32
LENGTH = 256


def draw_key_value_cache(key, part):
    drawn_values = jax.random.truncated_normal(key, -6.0, 6.0, (ROWS, LENGTH, 2 * HEAD), jnp.float32)
    return drawn_values.astype(jnp.bfloat16)


def with_ends(values, stream_key, low, high):
    shape = values.shape
    place = [jax.random.randint(jax.random.fold_in(stream_key, axis), (), 0, shape[axis]) for axis in range(len(shape))]
    values = values.at[tuple(place)].set(low)
    longest = shape.index(max(shape))
    place[longest] = (place[longest] + 1) % shape[longest]
    return values.at[tuple(place)].set(high)


def block_levels(own_key, dims, cuts, smallest, high):
    level = 1.0
    for dim, parts in cuts:
        heights = jax.random.uniform(jax.random.fold_in(jax.random.fold_in(own_key, 6), dim), (parts,), jnp.float32, smallest / len(cuts), high / len(cuts))
        level = level * jnp.repeat(jnp.exp(heights), dims[dim] // parts).reshape((-1,) + (1,) * (len(dims) - 1 - dim))
    return level


def distinct(stream_key, rows, count, top, lift):
    ranking = jax.random.permutation(jax.random.fold_in(stream_key, 1), count)
    boost = ranking
    for power in range(3):
        boost = boost * boost // count
    boost = boost * lift // count
    tickets = jax.random.randint(jax.random.fold_in(stream_key, 2), (rows, count), 0, 4096) + boost
    sure = jax.random.permutation(jax.random.fold_in(stream_key, 3), rows)[jnp.arange(count) % rows]
    tickets = jnp.where(jnp.arange(rows)[:, None] == sure[None, :], 1 << 14, tickets)
    priority = tickets * count + jnp.arange(count)
    return lax.top_k(priority.astype(jnp.int32), top)[1].astype(jnp.int32)


def normal_values(rng, dims, deviation, limit, pieces=(), held_as=jnp.bfloat16):
    entries = deviation * jax.random.normal(rng, dims, jnp.float32)
    if pieces:
        entries = entries * block_levels(rng, dims, pieces, -0.22, 0.18)
    return jnp.clip(entries, -limit, limit).astype(held_as)


def setup_inputs(seed: int = 0) -> dict:
    keys = jax.random.split(jax.random.key(seed), 10)
    return {
        "hidden": normal_values(keys[0], (STEPS, ROWS, D), 1.0, 6.0, ((1, 4),), jnp.float32),
        "norm_gain": jnp.clip(1.0 + 0.1 * jax.random.normal(keys[1], (D,), jnp.float32), 0.5, 1.5),
        "router": normal_values(keys[2], (D, EXPERTS), D ** -0.5, 0.0625),
        "key_value_weight": normal_values(keys[3], (D, 2 * HEAD), D ** -0.5, 0.0625),
        "query_master": normal_values(keys[4], (D, EXPERTS * HEAD), D ** -0.5, 0.0625, ((0, 4), (1, 8)), jnp.float32),
        "output_master": normal_values(keys[5], (D, EXPERTS * HEAD), (HEAD // 4) ** -0.5, 1.0, ((0, 4), (1, 8)), jnp.float32),
        "key_value_cache": draw_key_value_cache(jax.random.fold_in(keys[9], 71), 0),
        "lengths": with_ends(jax.random.randint(keys[7], (ROWS,), LENGTH // 4, LENGTH + 1), jax.random.fold_in(keys[7], 1), LENGTH // 4, LENGTH).astype(jnp.int32),
        "routes": distinct(keys[8], STEPS * ROWS, EXPERTS, TOPK, 4096).reshape((STEPS, ROWS, TOPK)),
    }


def reference(hidden, norm_gain, router, key_value_weight, query_master, output_master, key_value_cache, lengths, routes):
    mean_square = lax.optimization_barrier(jnp.mean(hidden * hidden, axis=-1, keepdims=True))
    normed = (hidden * lax.rsqrt(mean_square + 1e-05) * norm_gain).astype(jnp.bfloat16)
    flat_rows = normed.reshape(STEPS * ROWS, D)
    logits = jnp.dot(flat_rows, router, preferred_element_type=jnp.float32).reshape(STEPS, ROWS, EXPERTS)
    expert_ids = jnp.arange(EXPERTS).astype(jnp.int32)
    chosen = lax.optimization_barrier(jnp.sum((routes[..., None] == expert_ids).astype(jnp.float32), axis=2))
    picked = jax.nn.sigmoid(logits) * chosen
    gate_values = picked / lax.optimization_barrier(jnp.sum(picked, axis=-1, keepdims=True))
    fresh_pairs = jnp.dot(flat_rows, key_value_weight, preferred_element_type=jnp.float32).astype(jnp.bfloat16)
    fresh_float = fresh_pairs.reshape(STEPS, ROWS, 2 * HEAD).astype(jnp.float32)
    query_weight = query_master.astype(jnp.bfloat16)
    queries = jnp.dot(flat_rows, query_weight, preferred_element_type=jnp.float32).astype(jnp.bfloat16)
    queries = queries.reshape(STEPS, ROWS, EXPERTS, HEAD).astype(jnp.float32)
    cache_float = key_value_cache.astype(jnp.float32)
    score_factor = 1.0 / math.sqrt(HEAD)
    cache_scores = jnp.einsum('sreh,rph->srep', queries, cache_float[..., :HEAD]) * score_factor
    positions = jnp.arange(LENGTH).astype(jnp.int32)
    cache_mask = (positions[None, :] < lengths[:, None])[None, :, None, :]
    fresh_scores = jnp.einsum('sreh,urh->sreu', queries, fresh_float[..., :HEAD]) * score_factor
    step_order = jnp.arange(STEPS).astype(jnp.int32)
    fresh_mask = (step_order[None, :] <= step_order[:, None])[:, None, None, :]
    highest = jnp.maximum(lax.optimization_barrier(jnp.max(jnp.where(cache_mask, cache_scores, -jnp.inf), axis=-1)), lax.optimization_barrier(jnp.max(jnp.where(fresh_mask, fresh_scores, -jnp.inf), axis=-1)))
    cache_weights = jnp.where(cache_mask, jnp.exp(cache_scores - highest[..., None]), 0.0)
    fresh_weights = jnp.where(fresh_mask, jnp.exp(fresh_scores - highest[..., None]), 0.0)
    denominator = lax.optimization_barrier(jnp.sum(cache_weights, axis=-1)) + lax.optimization_barrier(jnp.sum(fresh_weights, axis=-1))
    mixture = jnp.einsum('srep,rph->sreh', cache_weights, cache_float[..., HEAD:])
    mixture = mixture + jnp.einsum('sreu,urh->sreh', fresh_weights, fresh_float[..., HEAD:])
    attended = (mixture / denominator[..., None]).astype(jnp.bfloat16)
    gated_rows = (gate_values[..., None] * attended.astype(jnp.float32)).reshape(STEPS * ROWS, EXPERTS * HEAD)
    output_rounded = lax.optimization_barrier(output_master.astype(jnp.bfloat16))
    output_float = output_rounded.astype(jnp.float32)
    projected = jnp.dot(gated_rows, output_float.T, precision=lax.Precision.HIGHEST)
    result = hidden + projected.reshape(STEPS, ROWS, D)
    return jnp.roll(result, ROWS_DEV, axis=1)
```

```python
import math

import jax
import jax.numpy as jnp
from jax import lax
from jax.sharding import PartitionSpec as P


BOTH = ("section", "head")


def exchange(pick, axis):
    count = lax.axis_size(axis)
    me = lax.axis_index(axis)
    if count > 4 or count & (count - 1):
        blocks = jnp.stack([pick(i) for i in range(count)])
        return lax.all_to_all(blocks, axis, 0, 0, tiled=True)
    arrived = [pick(me)]
    for offset in range(1, count):
        pairs = [(source, source ^ offset) for source in range(count)]
        arrived.append(lax.ppermute(pick(me ^ offset), axis, pairs))
    stacked = jnp.stack(arrived)
    return jnp.stack([lax.dynamic_index_in_dim(stacked, me ^ i, 0, False) for i in range(count)])


def split_three(values):
    pieces = []
    for _ in range(3):
        piece = lax.reduce_precision(values, 8, 7)
        pieces.append(piece.astype(jnp.bfloat16))
        values = values - piece
    return pieces


def body(
    hidden,
    norm_gain,
    router,
    key_value_weight,
    query_master,
    output_master,
    key_value_cache,
    lengths,
    routes,
):
    step_count, row_count, model_width = hidden.shape
    head_dim = key_value_weight.shape[1] // 2
    experts = router.shape[1]
    sections = lax.axis_size("section")
    heads = lax.axis_size("head")
    own_section = lax.axis_index("section")
    own_head = lax.axis_index("head")
    flat = step_count * row_count
    depth = model_width // sections
    share = model_width // heads
    part = share // sections
    per_section = heads // sections
    groups = heads // row_count
    own_steps = step_count // groups
    own_row = own_head // groups
    first_step = (own_head % groups) * own_steps

    slice_pairs = [(i, (i + 1) % sections) for i in range(sections)]
    hidden_slice = lax.ppermute(
        lax.dynamic_slice_in_dim(hidden, own_head * share, share, 2), "section", slice_pairs
    )
    cache_rows = lax.all_to_all(
        jnp.repeat(key_value_cache, groups, axis=0), "head", 0, 0, tiled=True
    )
    cache_rows = cache_rows.reshape(-1, 2 * head_dim)

    mean_square = jnp.mean(hidden * hidden, axis=-1, keepdims=True)
    normed = (hidden * lax.rsqrt(mean_square + 1e-05) * norm_gain).astype(jnp.bfloat16)
    flat_rows = normed.reshape(flat, model_width)
    every_row = exchange(
        lambda i: lax.dynamic_slice_in_dim(flat_rows, i * depth, depth, 1), "section"
    ).reshape(sections * flat, depth)

    output_piece = output_master.astype(jnp.bfloat16).reshape(per_section, sections, part, head_dim)
    quarters = exchange(
        lambda i: lax.dynamic_index_in_dim(output_piece, i, 1, False), "section"
    ).reshape(heads, part, head_dim)
    output_weight = lax.all_to_all(quarters, "head", 0, 0, tiled=True)

    logits = jnp.dot(flat_rows, router, preferred_element_type=jnp.float32).reshape(
        step_count, row_count, experts
    )
    chosen = jnp.sum((routes[..., None] == jnp.arange(experts)).astype(jnp.float32), axis=2)
    picked = jax.nn.sigmoid(logits) * chosen
    gate_values = picked / jnp.sum(picked, axis=-1, keepdims=True)
    own_gates = lax.dynamic_slice(
        gate_values, (first_step, own_row, 0), (own_steps, 1, experts)
    ).reshape(own_steps, experts)
    fresh_pairs = jnp.dot(flat_rows, key_value_weight, preferred_element_type=jnp.float32).astype(
        jnp.bfloat16
    )
    fresh_pairs = fresh_pairs.reshape(step_count, row_count, 2 * head_dim)
    fresh_pairs = lax.dynamic_index_in_dim(fresh_pairs, own_row, 1, False)
    key_new = fresh_pairs[:, :head_dim]
    value_new = fresh_pairs[:, head_dim:]

    partial = jnp.dot(
        every_row, query_master.astype(jnp.bfloat16), preferred_element_type=jnp.float32
    )
    partial = partial.reshape(sections, groups, own_steps, row_count, head_dim)
    partial = partial.transpose(0, 3, 1, 2, 4).reshape(sections * heads, own_steps, head_dim)
    partial = lax.all_to_all(partial, BOTH, 0, 0, tiled=True)
    queries = jnp.sum(partial.reshape(sections, heads, own_steps, head_dim), axis=0)
    queries = queries.astype(jnp.bfloat16)

    score_factor = 1.0 / math.sqrt(head_dim)
    steps = first_step + jnp.arange(own_steps)
    fresh_mask = (jnp.arange(step_count)[None, :] <= steps[:, None])[None]
    fresh_scores = (
        jnp.einsum("esh,uh->esu", queries, key_new, preferred_element_type=jnp.float32)
        * score_factor
    )
    own_length = lax.dynamic_index_in_dim(lengths, own_row, 0, False)
    cache_mask = (jnp.arange(cache_rows.shape[0]) < own_length)[None, None, :]
    cache_scores = (
        jnp.einsum(
            "esh,ph->esp", queries, cache_rows[:, :head_dim], preferred_element_type=jnp.float32
        )
        * score_factor
    )
    highest = jnp.maximum(
        jnp.max(jnp.where(cache_mask, cache_scores, -jnp.inf), axis=-1, keepdims=True),
        jnp.max(jnp.where(fresh_mask, fresh_scores, -jnp.inf), axis=-1, keepdims=True),
    )
    cache_weights = jnp.where(cache_mask, jnp.exp(cache_scores - highest), 0.0)
    fresh_weights = jnp.where(fresh_mask, jnp.exp(fresh_scores - highest), 0.0)
    mixture = jnp.einsum(
        "esp,ph->esh", cache_weights, cache_rows[:, head_dim:], preferred_element_type=jnp.float32
    ) + jnp.einsum("esu,uh->esh", fresh_weights, value_new, preferred_element_type=jnp.float32)
    denominator = jnp.sum(cache_weights, axis=-1, keepdims=True) + jnp.sum(
        fresh_weights, axis=-1, keepdims=True
    )
    attended = (mixture / denominator).astype(jnp.bfloat16)

    gate_pieces = jnp.concatenate(split_three(own_gates), axis=-1)
    gate_pieces = jnp.pad(gate_pieces, ((0, 0), (0, -gate_pieces.shape[1] % 128)))
    message = jnp.concatenate(
        [attended.transpose(1, 0, 2).reshape(own_steps, experts * head_dim), gate_pieces], axis=1
    )
    message = jnp.broadcast_to(message[None], (sections * heads,) + message.shape)
    arrived = lax.all_to_all(message, BOTH, 0, 0, tiled=True)
    arrived = arrived.reshape(sections, row_count, step_count, -1).transpose(0, 2, 1, 3)
    arrived = arrived.reshape(sections * flat, -1)
    every_attended = arrived[:, : experts * head_dim].reshape(-1, experts, head_dim)
    pieces = arrived[:, experts * head_dim : experts * (head_dim + 3)].astype(jnp.float32)
    every_gate = pieces[:, :experts] + pieces[:, experts : 2 * experts] + pieces[:, 2 * experts :]

    per_expert = jnp.einsum(
        "neh,efh->nef", every_attended, output_weight, preferred_element_type=jnp.float32
    )
    projected = jnp.sum(every_gate[..., None] * per_expert, axis=1).reshape(sections, flat, part)

    finished = exchange(
        lambda i: lax.dynamic_index_in_dim(projected, (i + sections - 1) % sections, 0, False),
        "section",
    )
    finished = finished.transpose(1, 0, 2).reshape(step_count, row_count, share)
    return hidden_slice + finished


def solution(mesh):
    return jax.shard_map(
        body,
        mesh=mesh,
        in_specs=(
            P(None, "section", None),
            P(),
            P(),
            P(),
            P("section", "head"),
            P("section", "head"),
            P("section", "head", None),
            P("section"),
            P(None, "section", None),
        ),
        out_specs=P(None, "section", "head"),
        check_vma=False,
    )
```

```python
import math

import jax
import jax.numpy as jnp
from jax import lax
from jax.sharding import PartitionSpec as P


def shift_pairs(count, offset, stride=1, size=None):
    size = count // stride if size is None else size
    if size & (size - 1) == 0:
        return [(i, i ^ (offset * stride)) for i in range(count)]
    pairs = []
    for i in range(count):
        digit = i // stride % size
        pairs.append((i, i + ((offset - digit) % size - digit) * stride))
    return pairs


def partner(digit, offset, size):
    return digit ^ offset if size & (size - 1) == 0 else (offset - digit) % size


def swap(pick, axis, stride, size):
    count = lax.axis_size(axis)
    digit = lax.axis_index(axis) // stride % size
    offsets = range(1, size) if size & (size - 1) == 0 else range(size)
    arrived = [(digit, pick(digit))] if size & (size - 1) == 0 else []
    for offset in offsets:
        other = partner(digit, offset, size)
        block = lax.ppermute(pick(other), axis, shift_pairs(count, offset, stride, size))
        arrived.append((other, block))
    return arrived


def in_order(arrived):
    out = jnp.zeros((len(arrived),) + arrived[0][1].shape, arrived[0][1].dtype)
    for member, block in arrived:
        out = lax.dynamic_update_index_in_dim(out, block, member, 0)
    return out


def split_three(values):
    pieces = []
    for _ in range(3):
        piece = lax.reduce_precision(values, 8, 7)
        pieces.append(piece.astype(jnp.bfloat16))
        values = values - piece
    return pieces


def body(
    hidden,
    norm_gain,
    router,
    key_value_weight,
    query_master,
    output_master,
    key_value_cache,
    lengths,
    routes,
):
    steps, row_count, model_width = hidden.shape
    head_dim = key_value_weight.shape[1] // 2
    experts = router.shape[1]
    sections = lax.axis_size("section")
    heads = lax.axis_size("head")
    own_section = lax.axis_index("section")
    own_head = lax.axis_index("head")
    flat = steps * row_count
    depth = model_width // sections
    share = model_width // heads
    part = share // sections
    per_section = heads // sections
    outer = math.gcd(row_count, heads // 2)
    inner = heads // outer
    rows = row_count // outer
    own_outer = own_head // inner
    own_inner = own_head % inner
    own_flat = steps * rows
    core = 2 if sections == 4 else 1

    query_piece = query_master.astype(jnp.bfloat16)
    if core == 2:
        far = lax.ppermute(query_piece, "section", shift_pairs(sections, 2))
        near = jnp.concatenate([query_piece, far], axis=0)
        near_other = lax.ppermute(near, "section", shift_pairs(sections, 1))
        query_blocks = [
            (own_section, near[:depth]),
            (own_section ^ 2, near[depth:]),
            (own_section ^ 1, near_other[:depth]),
            (own_section ^ 3, near_other[depth:]),
        ]
    else:
        query_all = lax.all_gather(query_piece, "section", axis=0, tiled=True)
        query_blocks = [(i, query_all[i * depth : (i + 1) * depth]) for i in range(sections)]

    cache_rows = key_value_cache.reshape((outer, 1, rows) + key_value_cache.shape[1:])
    cache_rows = jnp.broadcast_to(
        cache_rows, (outer, inner, rows) + key_value_cache.shape[1:]
    ).reshape((heads, rows) + key_value_cache.shape[1:])
    cache_rows = lax.all_to_all(cache_rows, "head", 0, 0, tiled=True)
    cache_rows = cache_rows.transpose(1, 0, 2, 3).reshape(rows, -1, 2 * head_dim)

    output_piece = output_master.astype(jnp.bfloat16).reshape(per_section, sections, part, head_dim)
    if core == 2:
        halves = output_piece.reshape(per_section, 2, 2, part, head_dim)
        x_digit = own_section // 2
        c_digit = own_section % 2
        far = lax.ppermute(
            lax.dynamic_index_in_dim(halves, 1 - x_digit, 1, False),
            "section",
            shift_pairs(sections, 2),
        )
        both = in_order(
            [(x_digit, lax.dynamic_index_in_dim(halves, x_digit, 1, False)), (1 - x_digit, far)]
        )
        near_other = lax.ppermute(
            lax.dynamic_index_in_dim(both, 1 - c_digit, 2, False),
            "section",
            shift_pairs(sections, 1),
        )
        parts = in_order(
            [(c_digit, lax.dynamic_index_in_dim(both, c_digit, 2, False)), (1 - c_digit, near_other)]
        )
        parts = parts.transpose(1, 0, 2, 3, 4)
    else:
        parts = lax.all_to_all(output_piece.transpose(1, 0, 2, 3), "section", 0, 0, tiled=True)
    output_weight = lax.all_to_all(parts.reshape(heads, part, head_dim), "head", 0, 0, tiled=True)

    hidden_slice = lax.ppermute(
        lax.dynamic_slice_in_dim(hidden, own_head * share, share, 2),
        "section",
        [(i, (i + 1) % sections) for i in range(sections)],
    )

    mean_square = jnp.mean(hidden * hidden, axis=-1, keepdims=True)
    normed = (hidden * lax.rsqrt(mean_square + 1e-05) * norm_gain).astype(jnp.bfloat16)
    flat_rows = normed.reshape(flat, model_width)

    queries = 0.0
    for index, block in query_blocks:
        rows_block = lax.dynamic_slice_in_dim(flat_rows, index * depth, depth, 1)
        queries = queries + jnp.dot(rows_block, block, preferred_element_type=jnp.float32)
    queries = lax.reduce_precision(queries, 8, 7)

    slab = model_width // outer
    slab_rows = lax.dynamic_slice_in_dim(flat_rows, own_outer * slab, slab, 1)
    fresh_part = jnp.dot(
        slab_rows,
        lax.dynamic_slice_in_dim(key_value_weight, own_outer * slab, slab, 0),
        preferred_element_type=jnp.float32,
    )
    logit_part = jnp.dot(
        slab_rows,
        lax.dynamic_slice_in_dim(router, own_outer * slab, slab, 0),
        preferred_element_type=jnp.float32,
    )
    logit_part = jnp.pad(logit_part, ((0, 0), (0, -experts % head_dim)))
    message = jnp.concatenate([queries, fresh_part, logit_part], axis=1)
    message = message.reshape(steps, outer, rows, -1).transpose(1, 0, 2, 3)
    arrived = swap(lambda i: lax.dynamic_index_in_dim(message, i, 0, False), "head", inner, outer)
    summed = sum(block[..., head_dim:] for _, block in arrived)
    fresh_pairs = summed[..., : 2 * head_dim].astype(jnp.bfloat16)
    logits = summed[..., 2 * head_dim : 2 * head_dim + experts]
    queries = in_order([(member, block[..., :head_dim]) for member, block in arrived])
    queries = queries.astype(jnp.bfloat16)
    key_new = fresh_pairs[..., :head_dim]
    value_new = fresh_pairs[..., head_dim:]

    own_routes = lax.dynamic_slice_in_dim(routes, own_outer * rows, rows, 1)
    chosen = jnp.sum((own_routes[..., None] == jnp.arange(experts)).astype(jnp.float32), axis=2)
    picked = jax.nn.sigmoid(logits) * chosen
    gates = picked / jnp.sum(picked, axis=-1, keepdims=True)
    gates = lax.dynamic_index_in_dim(
        gates.reshape(steps, rows, outer, inner), own_inner, 3, False
    ).reshape(own_flat, outer)

    score_factor = 1.0 / math.sqrt(head_dim)
    step_order = jnp.arange(steps)
    fresh_mask = (step_order[None, :] <= step_order[:, None])[None, None]
    fresh_scores = (
        jnp.einsum("esrh,urh->resu", queries, key_new, preferred_element_type=jnp.float32)
        * score_factor
    )
    own_lengths = lax.dynamic_slice_in_dim(lengths, own_outer * rows, rows, 0)
    cache_mask = (jnp.arange(cache_rows.shape[1])[None, :] < own_lengths[:, None])[:, None, None, :]
    cache_scores = (
        jnp.einsum(
            "esrh,rph->resp",
            queries,
            cache_rows[..., :head_dim],
            preferred_element_type=jnp.float32,
        )
        * score_factor
    )
    highest = jnp.maximum(
        jnp.max(jnp.where(cache_mask, cache_scores, -jnp.inf), axis=-1, keepdims=True),
        jnp.max(jnp.where(fresh_mask, fresh_scores, -jnp.inf), axis=-1, keepdims=True),
    )
    cache_weights = jnp.where(cache_mask, jnp.exp(cache_scores - highest), 0.0)
    fresh_weights = jnp.where(fresh_mask, jnp.exp(fresh_scores - highest), 0.0)
    mixture = jnp.einsum(
        "resp,rph->resh",
        cache_weights,
        cache_rows[..., head_dim:],
        preferred_element_type=jnp.float32,
    ) + jnp.einsum("resu,urh->resh", fresh_weights, value_new, preferred_element_type=jnp.float32)
    denominator = jnp.sum(cache_weights, axis=-1, keepdims=True) + jnp.sum(
        fresh_weights, axis=-1, keepdims=True
    )
    attended = (mixture / denominator).astype(jnp.bfloat16)

    gate_pieces = jnp.concatenate(split_three(gates), axis=-1)
    gate_pieces = jnp.pad(gate_pieces, ((0, 0), (0, -gate_pieces.shape[1] % 128)))
    attended = attended.transpose(2, 0, 1, 3).reshape(own_flat, outer * head_dim)
    message = jnp.concatenate([attended, gate_pieces], axis=1)
    if core == 2:
        from_sections = swap(lambda i: message, "section", 1, sections)
        message = jnp.stack([block for _, block in from_sections])
    else:
        message = lax.all_to_all(
            jnp.broadcast_to(message[None], (sections,) + message.shape), "section", 0, 0, tiled=True
        )
    message = in_order(swap(lambda i: message, "head", 1, inner))
    message = in_order(swap(lambda i: message, "head", inner, outer))
    message = message.reshape(outer, inner, sections, steps, rows, -1)
    width = outer * head_dim
    vectors = message[..., :width].reshape(outer, inner, sections, steps, rows, outer, head_dim)
    vectors = vectors.transpose(2, 3, 0, 4, 5, 1, 6).reshape(sections * flat, experts, head_dim)
    pieces = message[..., width : width + 3 * outer].astype(jnp.float32)
    every_gate = (
        pieces[..., :outer] + pieces[..., outer : 2 * outer] + pieces[..., 2 * outer :]
    )
    every_gate = every_gate.transpose(2, 3, 0, 4, 5, 1).reshape(sections * flat, experts)

    per_expert = jnp.einsum(
        "neh,efh->nef", vectors, output_weight, preferred_element_type=jnp.float32
    )
    projected = jnp.sum(every_gate[..., None] * per_expert, axis=1).reshape(sections, flat, part)

    def group_of(member):
        return (member + sections - 1) % sections

    if core == 2:
        finished = in_order(
            swap(
                lambda i: lax.dynamic_index_in_dim(projected, group_of(i) ^ own_section, 0, False),
                "section",
                1,
                sections,
            )
        )
    else:
        finished = lax.all_to_all(
            jnp.roll(projected, 1, axis=0), "section", 0, 0, tiled=True
        )
    finished = finished.transpose(1, 0, 2).reshape(steps, row_count, share)
    return hidden_slice + finished


def solution(mesh):
    return jax.shard_map(
        body,
        mesh=mesh,
        in_specs=(
            P(None, "section", None),
            P(),
            P(),
            P(),
            P("section", "head"),
            P("section", "head"),
            P("section", "head", None),
            P("section"),
            P(None, "section", None),
        ),
        out_specs=P(None, "section", "head"),
        check_vma=False,
    )
```
